8 devices in a mesh: t: 4 (over z, y, x), v: 2 (over core).
Axes of the slice: x: 2, y: 2, z: 1, core: 2. Of those that a mesh axis runs over, the one named last changes fastest.
Arguments:
- hidden_in: bfloat16 [512, 2560], replicated
- seq_lens: int32 [512], replicated
- target: int32 [512], replicated
- g_attn_pre: bfloat16 [2560], replicated
- w_q: bfloat16 [2560, 2048], P(None, 't')
- w_k: bfloat16 [2560, 1024], P(None, 't')
- w_v: bfloat16 [2560, 1024], P(None, 't')
- w_o: bfloat16 [2048, 2560], P('t')
- g_attn_post: bfloat16 [2560], replicated
- g_mlp_pre: bfloat16 [2560], replicated
- w_gate: bfloat16 [2560, 10240], P(None, 't')
- w_up: bfloat16 [2560, 10240], P(None, 't')
- w_down: bfloat16 [10240, 2560], P('t')
- g_mlp_post: bfloat16 [2560], replicated
- g_final: bfloat16 [2560], replicated
- k_cache: bfloat16 [512, 32, 4, 256], P(None, None, 't')
- v_cache: bfloat16 [512, 32, 4, 256], P(None, None, 't')
- embed_table: bfloat16 [262144, 2560], P(('v', 't'))
Outputs:
- output 1: float32 [512], replicated
- output 2: bfloat16 [512, 2560], replicated
All inputs are finite; a program needn't handle non-finite values.
Results may differ from the reference program's by a relative error of at most 0.00777438.
Values sent between devices are 32-bit elements.
A program may use at most 1 GiB of HBM per device.

```python
import jax
import jax.numpy as jnp
from jax import lax

D = 2560
HEADS = 8
KV_HEADS = 4
HEAD = 256
FF = 10240
VOCAB = 262144
TOKENS = 512
CTX = 32

ATTN_CAP = 50.0
FINAL_CAP = 30.0
NORM_EPS = 1e-6
ROPE_BASE = 10000.0


def rms_norm(values, gain_vec):
    x_f32 = values.astype(jnp.float32)
    scaled = x_f32 * lax.rsqrt(jnp.mean(x_f32 * x_f32, axis=-1, keepdims=True) + NORM_EPS)
    return scaled * (1.0 + gain_vec.astype(jnp.float32))


def rotary(values, positions):
    half_dim = values.shape[-1] // 2
    inv_freq = ROPE_BASE ** (-2.0 * jnp.arange(half_dim, dtype=jnp.float32) / values.shape[-1])
    angles = positions.astype(jnp.float32)[:, None] * inv_freq[None, :]
    angles = angles.reshape((values.shape[0],) + (1,) * (values.ndim - 2) + (half_dim,))
    cos_t = jnp.cos(angles)
    sin_t = jnp.sin(angles)
    x_low = values[..., :half_dim]
    x_high = values[..., half_dim:]
    return jnp.concatenate([x_low * cos_t - x_high * sin_t, x_high * cos_t + x_low * sin_t], axis=-1)


def setup_inputs(seed: int = 0) -> dict:
    keys = jax.random.split(jax.random.key(seed), 20)

    def normal_draw(sub_key, dims, scale_by):
        return (jax.random.normal(sub_key, dims, jnp.float32) * scale_by).astype(jnp.bfloat16)

    int_keys = jax.random.split(keys[19], 4)
    token_ids = jnp.arange(TOKENS)
    seq_lens = jax.random.randint(int_keys[0], (TOKENS,), 1, CTX + 1)
    picked = jax.random.permutation(int_keys[1], TOKENS)
    seq_lens = jnp.where(token_ids == picked[0], CTX, seq_lens)
    seq_lens = jnp.where(token_ids == picked[1], 1, seq_lens).astype(jnp.int32)
    stride = VOCAB // TOKENS
    target = token_ids * stride + jax.random.randint(int_keys[2], (TOKENS,), 0, stride)
    target = jax.random.permutation(int_keys[3], target).astype(jnp.int32)
    d_scale = D ** -0.5
    return {
        'hidden_in': normal_draw(keys[0], (TOKENS, D), 1.0),
        'seq_lens': seq_lens,
        'target': target,
        'g_attn_pre': normal_draw(keys[1], (D,), 0.4),
        'w_q': normal_draw(keys[2], (D, HEADS * HEAD), 4.0 * d_scale),
        'w_k': normal_draw(keys[3], (D, KV_HEADS * HEAD), 4.0 * d_scale),
        'w_v': normal_draw(keys[4], (D, KV_HEADS * HEAD), d_scale),
        'w_o': normal_draw(keys[5], (HEADS * HEAD, D), (HEADS * HEAD) ** -0.5),
        'g_attn_post': normal_draw(keys[6], (D,), 0.4),
        'g_mlp_pre': normal_draw(keys[7], (D,), 0.4),
        'w_gate': normal_draw(keys[8], (D, FF), d_scale),
        'w_up': normal_draw(keys[9], (D, FF), d_scale),
        'w_down': normal_draw(keys[10], (FF, D), FF ** -0.5),
        'g_mlp_post': normal_draw(keys[11], (D,), 0.4),
        'g_final': normal_draw(keys[12], (D,), 0.4),
        'k_cache': normal_draw(keys[13], (TOKENS, CTX, KV_HEADS, HEAD), 4.0),
        'v_cache': normal_draw(keys[14], (TOKENS, CTX, KV_HEADS, HEAD), 1.0),
        'embed_table': normal_draw(keys[15], (VOCAB, D), 25.0 * d_scale),
    }


def reference(hidden_in, seq_lens, target, g_attn_pre, w_q, w_k, w_v, w_o, g_attn_post, g_mlp_pre, w_gate, w_up, w_down, g_mlp_post, g_final, k_cache, v_cache, embed_table):
    group_size = HEADS // KV_HEADS
    score_scale = HEAD ** -0.5
    normed = rms_norm(hidden_in, g_attn_pre).astype(jnp.bfloat16)
    q_rot = rotary(jnp.dot(normed, w_q, preferred_element_type=jnp.float32).reshape(TOKENS, KV_HEADS, group_size, HEAD), seq_lens).astype(jnp.bfloat16)
    k_rot = rotary(jnp.dot(normed, w_k, preferred_element_type=jnp.float32).reshape(TOKENS, KV_HEADS, HEAD), seq_lens).astype(jnp.bfloat16)
    v_new = jnp.dot(normed, w_v, preferred_element_type=jnp.float32).astype(jnp.bfloat16).reshape(TOKENS, KV_HEADS, HEAD)

    def attend(operands):
        q_tok, k_tok, v_tok, keys_tok, vals_tok, len_tok = operands
        q_f32 = q_tok.astype(jnp.float32)
        s_cache = jnp.einsum('kgd,tkd->kgt', q_f32, keys_tok.astype(jnp.float32)) * score_scale
        s_new = jnp.einsum('kgd,kd->kg', q_f32, k_tok.astype(jnp.float32)) * score_scale
        s_cache = ATTN_CAP * jnp.tanh(s_cache / ATTN_CAP)
        s_new = ATTN_CAP * jnp.tanh(s_new / ATTN_CAP)
        s_cache = jnp.where(jnp.arange(CTX) < len_tok, s_cache, -1e30)
        row_max = jnp.maximum(jnp.max(s_cache, axis=-1), s_new)
        p_cache = jnp.exp(s_cache - row_max[..., None])
        p_new = jnp.exp(s_new - row_max)
        denominator = jnp.sum(p_cache, axis=-1) + p_new
        weighted = jnp.einsum('kgt,tkd->kgd', p_cache.astype(jnp.bfloat16).astype(jnp.float32), vals_tok.astype(jnp.float32))
        weighted = weighted + p_new.astype(jnp.bfloat16).astype(jnp.float32)[..., None] * v_tok.astype(jnp.float32)[:, None, :]
        return (weighted / denominator[..., None]).astype(jnp.bfloat16)

    attn_vec = lax.map(attend, (q_rot, k_rot, v_new, k_cache, v_cache, seq_lens))
    attn_out = jnp.dot(attn_vec.reshape(TOKENS, HEADS * HEAD), w_o, preferred_element_type=jnp.float32)
    hidden_mid = (hidden_in.astype(jnp.float32) + rms_norm(attn_out, g_attn_post)).astype(jnp.bfloat16)
    mlp_in = rms_norm(hidden_mid, g_mlp_pre).astype(jnp.bfloat16)
    gate_proj = jnp.dot(mlp_in, w_gate, preferred_element_type=jnp.float32)
    up_proj = jnp.dot(mlp_in, w_up, preferred_element_type=jnp.float32)
    activated = (jax.nn.gelu(gate_proj, approximate=True) * up_proj).astype(jnp.bfloat16)
    mlp_out = jnp.dot(activated, w_down, preferred_element_type=jnp.float32)
    hidden_out = (hidden_mid.astype(jnp.float32) + rms_norm(mlp_out, g_mlp_post)).astype(jnp.bfloat16)
    final_h = rms_norm(hidden_out, g_final).astype(jnp.bfloat16)

    blocks = 16
    block_rows = VOCAB // blocks
    table_blocks = embed_table.reshape(blocks, block_rows, D)
    starts = jnp.arange(blocks) * block_rows

    def block_stats(operands):
        table_block, start_row = operands
        logits = jnp.dot(final_h, table_block.T, preferred_element_type=jnp.float32)
        capped = FINAL_CAP * jnp.tanh(logits / FINAL_CAP)
        block_max = jnp.max(capped, axis=1)
        block_sum = jnp.sum(jnp.exp(capped - block_max[:, None]), axis=1)
        hit_mask = (start_row + jnp.arange(block_rows))[None, :] == target[:, None]
        block_tgt = jnp.sum(jnp.where(hit_mask, capped, 0.0), axis=1)
        return block_max, block_sum, block_tgt

    all_max, all_sum, all_tgt = lax.map(block_stats, (table_blocks, starts))
    glob_max = jnp.max(all_max, axis=0)
    log_norm = glob_max + jnp.log(jnp.sum(all_sum * jnp.exp(all_max - glob_max[None, :]), axis=0))
    logprob = jnp.sum(all_tgt, axis=0) - log_norm
    return logprob, hidden_out
```

```python
import jax
import jax.numpy as jnp
from jax import lax
from jax.experimental import pallas as pl
from jax.experimental.pallas import tpu as pltpu
from jax.sharding import PartitionSpec as P

ATTN_CAP = 50.0
FINAL_CAP = 30.0
NORM_EPS = 1e-6
ROPE_BASE = 10000.0


def rms_norm(values, gain_vec):
    x_f32 = values.astype(jnp.float32)
    scaled = x_f32 * lax.rsqrt(jnp.mean(x_f32 * x_f32, axis=-1, keepdims=True) + NORM_EPS)
    return scaled * (1.0 + gain_vec.astype(jnp.float32))


def rotary(values, positions):
    half_dim = values.shape[-1] // 2
    inv_freq = ROPE_BASE ** (-2.0 * jnp.arange(half_dim, dtype=jnp.float32) / values.shape[-1])
    angles = positions.astype(jnp.float32)[:, None] * inv_freq[None, :]
    angles = angles.reshape((values.shape[0],) + (1,) * (values.ndim - 2) + (half_dim,))
    cos_t = jnp.cos(angles)
    sin_t = jnp.sin(angles)
    x_low = values[..., :half_dim]
    x_high = values[..., half_dim:]
    return jnp.concatenate([x_low * cos_t - x_high * sin_t, x_high * cos_t + x_low * sin_t], axis=-1)


def attention(normed, seq_lens, w_q, w_k, w_v, k_cache, v_cache):
    tokens, ctx_len, kv_heads, head_dim = k_cache.shape
    group_size = w_q.shape[1] // (kv_heads * head_dim)
    score_scale = head_dim ** -0.5
    q_rot = rotary(jnp.dot(normed, w_q, preferred_element_type=jnp.float32).reshape(tokens, kv_heads, group_size, head_dim), seq_lens).astype(jnp.bfloat16)
    k_rot = rotary(jnp.dot(normed, w_k, preferred_element_type=jnp.float32).reshape(tokens, kv_heads, head_dim), seq_lens).astype(jnp.bfloat16)
    v_new = jnp.dot(normed, w_v, preferred_element_type=jnp.float32).astype(jnp.bfloat16).reshape(tokens, kv_heads, head_dim)
    s_cache = jnp.einsum('nkgd,ntkd->nkgt', q_rot, k_cache, preferred_element_type=jnp.float32) * score_scale
    s_new = jnp.einsum('nkgd,nkd->nkg', q_rot, k_rot, preferred_element_type=jnp.float32) * score_scale
    s_cache = ATTN_CAP * jnp.tanh(s_cache / ATTN_CAP)
    s_new = ATTN_CAP * jnp.tanh(s_new / ATTN_CAP)
    valid_mask = jnp.arange(ctx_len)[None, :] < seq_lens[:, None]
    s_cache = jnp.where(valid_mask[:, None, None, :], s_cache, -1e30)
    row_max = jnp.maximum(jnp.max(s_cache, axis=-1), s_new)
    p_cache = jnp.exp(s_cache - row_max[..., None])
    p_new = jnp.exp(s_new - row_max)
    denominator = jnp.sum(p_cache, axis=-1) + p_new
    weighted = jnp.einsum('nkgt,ntkd->nkgd', p_cache.astype(jnp.bfloat16), v_cache, preferred_element_type=jnp.float32)
    weighted = weighted + p_new.astype(jnp.bfloat16).astype(jnp.float32)[..., None] * v_new.astype(jnp.float32)[:, :, None, :]
    return (weighted / denominator[..., None]).astype(jnp.bfloat16).reshape(tokens, kv_heads * group_size * head_dim)


HEAD_ROWS = 2048
HEAD_SUB = 256


def head_kernel(base_ref, h_ref, tgt_ref, table_ref, sum_ref, hit_ref):
    step = pl.program_id(0)

    @pl.when(step == 0)
    def _():
        sum_ref[...] = jnp.zeros_like(sum_ref)
        hit_ref[...] = jnp.zeros_like(hit_ref)

    total = sum_ref[...]
    hit = hit_ref[...]
    target = tgt_ref[...] - (base_ref[0] + step * HEAD_ROWS)
    tokens = total.shape[1]
    for part in range(HEAD_ROWS // HEAD_SUB):
        rows = table_ref[part * HEAD_SUB:(part + 1) * HEAD_SUB, :]
        logits = jnp.dot(rows, h_ref[...], preferred_element_type=jnp.float32)
        capped = FINAL_CAP * jnp.tanh(logits / FINAL_CAP)
        row_ids = lax.broadcasted_iota(jnp.int32, logits.shape, 0) + part * HEAD_SUB
        total = total + jnp.sum(jnp.exp(capped).reshape(HEAD_SUB // 8, 8, tokens), axis=0)
        picked = jnp.where(row_ids == target, capped, 0.0)
        hit = hit + jnp.sum(picked.reshape(HEAD_SUB // 8, 8, tokens), axis=0)
    sum_ref[...] = total
    hit_ref[...] = hit


def head_sums(base, h_cols, target, table):
    width, tokens = h_cols.shape
    vocab = table.shape[0]
    return pl.pallas_call(
        head_kernel,
        grid=(vocab // HEAD_ROWS,),
        in_specs=[
            pl.BlockSpec(memory_space=pltpu.SMEM),
            pl.BlockSpec((width, tokens), lambda i: (0, 0)),
            pl.BlockSpec((1, tokens), lambda i: (0, 0)),
            pl.BlockSpec((HEAD_ROWS, width), lambda i: (i, 0)),
        ],
        out_specs=[pl.BlockSpec((8, tokens), lambda i: (0, 0))] * 2,
        out_shape=[jax.ShapeDtypeStruct((8, tokens), jnp.float32)] * 2,
        compiler_params=pltpu.CompilerParams(vmem_limit_bytes=56 * 2**20),
        name='head_sums',
    )(base, h_cols, target, table)


def solution(mesh):
    tp_size = mesh.shape['t']
    in_specs = (P(), P(), P(), P(), P(None, 't'), P(None, 't'), P(None, 't'), P('t', None), P(), P(), P(None, 't'), P(None, 't'), P('t', None), P(), P(), P(None, None, 't', None), P(None, None, 't', None), P(('v', 't'), None))

    def local_step(hidden_in, seq_lens, target, g_attn_pre, w_q, w_k, w_v, w_o, g_attn_post, g_mlp_pre, w_gate, w_up, w_down, g_mlp_post, g_final, k_cache, v_cache, embed_table):
        half = hidden_in.shape[0] // 2
        core = lax.axis_index('v')
        first = core * half
        all_tokens = hidden_in
        hidden_in = lax.dynamic_slice_in_dim(all_tokens, first, half, 0)
        seq_lens = lax.dynamic_slice_in_dim(seq_lens, first, half, 0)
        k_cache = lax.dynamic_slice_in_dim(k_cache, first, half, 0)
        v_cache = lax.dynamic_slice_in_dim(v_cache, first, half, 0)
        normed = rms_norm(hidden_in, g_attn_pre).astype(jnp.bfloat16)
        attn_vec = attention(normed, seq_lens, w_q, w_k, w_v, k_cache, v_cache)
        attn_part = jnp.dot(attn_vec, w_o, preferred_element_type=jnp.float32)
        attn_out = lax.psum(attn_part, 't')
        hidden_mid = (hidden_in.astype(jnp.float32) + rms_norm(attn_out, g_attn_post)).astype(jnp.bfloat16)
        mlp_in = rms_norm(hidden_mid, g_mlp_pre).astype(jnp.bfloat16)
        gate_proj = jnp.dot(mlp_in, w_gate, preferred_element_type=jnp.float32)
        up_proj = jnp.dot(mlp_in, w_up, preferred_element_type=jnp.float32)
        activated = (jax.nn.gelu(gate_proj, approximate=True) * up_proj).astype(jnp.bfloat16)
        mlp_part = jnp.dot(activated, w_down, preferred_element_type=jnp.float32)
        mlp_out = lax.psum(mlp_part, 't')
        half_out = (hidden_mid.astype(jnp.float32) + rms_norm(mlp_out, g_mlp_post)).astype(jnp.bfloat16)
        full_out = lax.all_gather(half_out.astype(jnp.float32), 'v', tiled=True)
        final_h = rms_norm(full_out, g_final).astype(jnp.bfloat16)
        hidden_out = full_out.astype(jnp.bfloat16)
        vocab_local = embed_table.shape[0]
        shard_index = core * tp_size + lax.axis_index('t')
        base = (shard_index * vocab_local).astype(jnp.int32).reshape(1)
        local_sum, local_hit = head_sums(base, final_h.T, target[None, :], embed_table)
        stats = jnp.stack([jnp.sum(local_sum, axis=0), jnp.sum(local_hit, axis=0)])
        stats = lax.psum(stats, ('v', 't'))
        logprob = stats[1] - jnp.log(stats[0])
        return logprob, hidden_out

    return jax.shard_map(local_step, mesh=mesh, in_specs=in_specs, out_specs=(P(), P()), check_vma=False)
```

```python
import jax
import jax.numpy as jnp
from jax import lax
from jax.experimental import pallas as pl
from jax.experimental.pallas import tpu as pltpu
from jax.sharding import PartitionSpec as P

ATTN_CAP = 50.0
FINAL_CAP = 30.0
NORM_EPS = 1e-6
ROPE_BASE = 10000.0


def rms_norm(values, gain_vec):
    x_f32 = values.astype(jnp.float32)
    scaled = x_f32 * lax.rsqrt(jnp.mean(x_f32 * x_f32, axis=-1, keepdims=True) + NORM_EPS)
    return scaled * (1.0 + gain_vec.astype(jnp.float32))


def rotary(values, positions):
    half_dim = values.shape[-1] // 2
    inv_freq = ROPE_BASE ** (-2.0 * jnp.arange(half_dim, dtype=jnp.float32) / values.shape[-1])
    angles = positions.astype(jnp.float32)[:, None] * inv_freq[None, :]
    angles = angles.reshape((values.shape[0],) + (1,) * (values.ndim - 2) + (half_dim,))
    cos_t = jnp.cos(angles)
    sin_t = jnp.sin(angles)
    x_low = values[..., :half_dim]
    x_high = values[..., half_dim:]
    return jnp.concatenate([x_low * cos_t - x_high * sin_t, x_high * cos_t + x_low * sin_t], axis=-1)


def attention(normed, seq_lens, w_q, w_k, w_v, k_cache, v_cache):
    tokens, ctx_len, kv_heads, head_dim = k_cache.shape
    group_size = w_q.shape[1] // (kv_heads * head_dim)
    score_scale = head_dim ** -0.5
    q_rot = rotary(jnp.dot(normed, w_q, preferred_element_type=jnp.float32).reshape(tokens, kv_heads, group_size, head_dim), seq_lens).astype(jnp.bfloat16)
    k_rot = rotary(jnp.dot(normed, w_k, preferred_element_type=jnp.float32).reshape(tokens, kv_heads, head_dim), seq_lens).astype(jnp.bfloat16)
    v_new = jnp.dot(normed, w_v, preferred_element_type=jnp.float32).astype(jnp.bfloat16).reshape(tokens, kv_heads, head_dim)
    s_cache = jnp.einsum('nkgd,ntkd->nkgt', q_rot, k_cache, preferred_element_type=jnp.float32) * score_scale
    s_new = jnp.einsum('nkgd,nkd->nkg', q_rot, k_rot, preferred_element_type=jnp.float32) * score_scale
    s_cache = ATTN_CAP * jnp.tanh(s_cache / ATTN_CAP)
    s_new = ATTN_CAP * jnp.tanh(s_new / ATTN_CAP)
    valid_mask = jnp.arange(ctx_len)[None, :] < seq_lens[:, None]
    s_cache = jnp.where(valid_mask[:, None, None, :], s_cache, -1e30)
    row_max = jnp.maximum(jnp.max(s_cache, axis=-1), s_new)
    p_cache = jnp.exp(s_cache - row_max[..., None])
    p_new = jnp.exp(s_new - row_max)
    denominator = jnp.sum(p_cache, axis=-1) + p_new
    weighted = jnp.einsum('nkgt,ntkd->nkgd', p_cache.astype(jnp.bfloat16), v_cache, preferred_element_type=jnp.float32)
    weighted = weighted + p_new.astype(jnp.bfloat16).astype(jnp.float32)[..., None] * v_new.astype(jnp.float32)[:, :, None, :]
    return (weighted / denominator[..., None]).astype(jnp.bfloat16).reshape(tokens, kv_heads * group_size * head_dim)


FIRST_GROUPS = 11
MESH = pl.DeviceIdType.MESH
BLOCK = 16
TILE = 512
SLOTS = 15
GROUP = 4
SUB = 256
CHUNKS = 2


def norm_rows(values, gain):
    return values * lax.rsqrt(jnp.mean(values * values, axis=-1, keepdims=True) + NORM_EPS) * (1.0 + gain)


def layer_head_kernel(
    part_hbm, x_hbm, tgt_ref, g_attn_ref, g_pre_ref, g_post_ref, g_final_ref, wg, wu, wd, table,
    logprob_ref, y_hbm,
    ring, part, landed, gat, oth, h, stage, act, mlp_in, xown, x1, zbuf, acc_sum, acc_hit, stats, stats_in,
    load_sem, part_sem, x_sem, y_sem, send_sem, recv_sem, pair_send, pair_recv, stat_send, stat_recv,
):
    t = lax.axis_index('t')
    v = lax.axis_index('v')
    x, y = lax.rem(t, 2), lax.div(t, 2)
    to_x = {'t': t + 1 - 2 * x}
    to_y = {'t': t + 2 - 4 * y}
    to_pair = {'v': 1 - v}
    half = part.shape[0]
    rows = half // CHUNKS
    vocab = table.shape[0]
    tiles = vocab // TILE
    base = (v * 4 + t) * vocab

    def b1(c, xo, yo):
        return c * rows + (xo * 2 + yo) * BLOCK

    def b2(c, yo, xo):
        return c * rows + rows // 2 + (yo * 2 + xo) * BLOCK

    def at(ref, row):
        return ref.at[pl.ds(pl.multiple_of(row, BLOCK), BLOCK), :]

    def remote(src, dst, send, recv, device):
        return pltpu.make_async_remote_copy(src_ref=src, dst_ref=dst, send_sem=send, recv_sem=recv, device_id=device, device_id_type=MESH)

    def weight_loads():
        out = []
        for n, w in enumerate((wg, wu, wd)):
            for k in range(5):
                slot = n * 5 + k
                out.append(pltpu.make_async_copy(w.at[pl.ds(k * TILE, TILE), :], ring.at[pl.ds(slot * TILE, TILE), :], load_sem.at[slot]))
        return out

    def table_load(q):
        slot = lax.rem(q, SLOTS)
        row = pl.multiple_of(lax.rem(q, tiles) * TILE, TILE)
        return pltpu.make_async_copy(table.at[pl.ds(row, TILE), :], ring.at[pl.ds(pl.multiple_of(slot * TILE, TILE), TILE), :], load_sem.at[slot])

    def scatter_copies(c, phase):
        s, r = send_sem.at[phase, c], recv_sem.at[phase, c]
        return (
            remote(at(part, b1(c, 1 - x, 1 - y)), landed.at[c, 0], s.at[0], r.at[0], to_x),
            remote(at(part, b1(c, 1 - x, y)), landed.at[c, 1], s.at[1], r.at[1], to_x),
            remote(at(part, b1(c, x, 1 - y)), landed.at[c, 2], s.at[2], r.at[2], to_y),
            remote(at(part, b2(c, 1 - y, 1 - x)), landed.at[c, 3], s.at[3], r.at[3], to_y),
            remote(at(part, b2(c, 1 - y, x)), landed.at[c, 4], s.at[4], r.at[4], to_y),
            remote(at(part, b2(c, y, 1 - x)), landed.at[c, 5], s.at[5], r.at[5], to_x),
        )

    def gather_copies(c, phase):
        s, r = send_sem.at[phase, c], recv_sem.at[phase, c]

        def same(row, k, device):
            return remote(at(gat, row), at(gat, row), s.at[k], r.at[k], device)

        return (
            same(b1(c, x, y), 0, to_y),
            same(b1(c, x, y), 1, to_x),
            same(b1(c, x, 1 - y), 2, to_x),
            same(b2(c, y, x), 3, to_x),
            same(b2(c, y, x), 4, to_y),
            same(b2(c, y, 1 - x), 5, to_y),
        )

    def scatter_start(c, phase):
        copies = scatter_copies(c, phase)
        for k in (0, 3, 1, 4):
            copies[k].start()

    def scatter_forward(c, phase):
        copies = scatter_copies(c, phase)
        for k, row in ((0, b1(c, x, 1 - y)), (3, b2(c, y, 1 - x))):
            copies[k].wait_recv()
            dst = at(part, row)
            dst[...] = dst[...] + landed[c, k]
            copies[k + 2].start()

    def scatter_finish_gather_start(c, phase):
        copies = scatter_copies(c, phase)
        out = gather_copies(c, phase + 1)
        for side, (k, row) in enumerate(((0, b1(c, x, y)), (3, b2(c, y, x)))):
            copies[k + 1].wait_recv()
            copies[k + 2].wait_recv()
            total = at(part, row)[...] + landed[c, k + 1] + landed[c, k + 2]
            mine = c * 2 + side
            if phase == 0:
                if c == 0 and side == 0:
                    for i in range(2 * CHUNKS):
                        own_x(i).wait()
                mid = (xown[mine].astype(jnp.float32) + norm_rows(total, g_attn_ref[...])).astype(jnp.bfloat16)
                x1[mine] = mid
                value = norm_rows(mid.astype(jnp.float32), g_pre_ref[...])
            else:
                value = x1[mine].astype(jnp.float32) + norm_rows(total, g_post_ref[...])
            at(gat, row)[...] = value.astype(jnp.bfloat16).astype(jnp.float32)
            out[k].start()
            out[k + 1].start()

    def gather_forward(c, phase):
        copies = gather_copies(c, phase)
        for k in (0, 3):
            copies[k].wait_recv()
            copies[k + 2].start()

    def gather_finish(c, phase):
        copies = gather_copies(c, phase)
        for k in (1, 2, 4, 5):
            copies[k].wait_recv()

    def drain(c, phase):
        for copy in scatter_copies(c, phase) + gather_copies(c, phase + 1):
            copy.wait_send()

    def own_x(i):
        c, side = i // 2, i % 2
        row = (b1(c, x, y), b2(c, y, x))[side] + v * half
        return pltpu.make_async_copy(at(x_hbm, row), xown.at[i], x_sem.at[i])

    def mlp(c, last):
        loads = weight_loads()
        mlp_in[...] = gat[c * rows:(c + 1) * rows, :].astype(jnp.bfloat16)
        for k in range(10):
            loads[k].wait()

        def gate_up(n, carry):
            cols = pl.ds(pl.multiple_of(n * TILE, TILE), TILE)
            gate = jnp.dot(mlp_in[...], ring[0:2560, cols], preferred_element_type=jnp.float32)
            up = jnp.dot(mlp_in[...], ring[2560:5120, cols], preferred_element_type=jnp.float32)
            act[:, cols] = (jax.nn.gelu(gate, approximate=True) * up).astype(jnp.bfloat16)
            return carry

        lax.fori_loop(0, 5, gate_up, 0)
        for k in range(10):
            if last:
                table_load(k).start()
            else:
                loads[k].start()
        for k in range(10, 15):
            loads[k].wait()
        drain(c, 0)

        def down(n, carry):
            cols = pl.ds(pl.multiple_of(n * TILE, TILE), TILE)
            part[c * rows:(c + 1) * rows, cols] = jnp.dot(act[...], ring[5120:7680, cols], preferred_element_type=jnp.float32)
            return carry

        lax.fori_loop(0, 5, down, 0)
        for k in range(10, 15):
            if last:
                table_load(k).start()
            else:
                loads[k].start()

    def pair_copy(c):
        span = pl.ds(c * rows, rows)
        return remote(gat.at[span, :], oth.at[span, :], pair_send.at[c], pair_recv.at[c], to_pair)

    def y_copies(c):
        out = []
        for k, owner in enumerate((v, 1 - v)):
            dst = y_hbm.at[pl.ds(pl.multiple_of(owner * half + c * rows, BLOCK), rows), :]
            out.append(pltpu.make_async_copy(stage.at[pl.ds(k * rows, rows), :], dst, y_sem.at[c, k]))
        return out

    def final_norm(c):
        pair = pair_copy(c)
        if c > 0:
            for copy in y_copies(c - 1):
                copy.wait()
        for k, (src, owner) in enumerate(((gat, v), (oth, 1 - v))):
            if k == 1:
                pair.wait_recv()

            def body(i, carry):
                row = pl.multiple_of(i * BLOCK, BLOCK)
                value = src[pl.ds(c * rows + row, BLOCK), :]
                stage[pl.ds(k * rows + row, BLOCK), :] = value.astype(jnp.bfloat16)
                h[pl.ds(pl.multiple_of((c * 2 + owner) * rows + row, BLOCK), BLOCK), :] = norm_rows(value, g_final_ref[...]).astype(jnp.bfloat16)
                return carry

            lax.fori_loop(0, rows // BLOCK, body, 0)
            y_copies(c)[k].start()

    def reduce_logits(logits, first_row, lo, width, keep):
        capped = FINAL_CAP * jnp.tanh(logits / FINAL_CAP)
        row_ids = lax.broadcasted_iota(jnp.int32, logits.shape, 0)
        wanted = tgt_ref[:, lo:lo + width] - (base + first_row)
        total = jnp.sum(jnp.exp(capped).reshape(SUB // 8, 8, width), axis=0)
        hit = jnp.sum(jnp.where(row_ids == wanted, capped, 0.0).reshape(SUB // 8, 8, width), axis=0)
        if keep is not None:
            total = jnp.where(keep, total, 0.0)
            hit = jnp.where(keep, hit, 0.0)
        acc_sum[:, lo:lo + width] += total
        acc_hit[:, lo:lo + width] += hit

    def head(first, last, lo, width, total_tiles, opens, closes):
        def body(g, carry):
            q0 = g * GROUP
            for k in range(GROUP):
                table_load(q0 + k).wait()
            pending = zbuf[:, 0:width]
            pending_row = lax.rem(q0, tiles) * TILE - SUB
            keep = g > first if opens else None
            for k in range(GROUP):
                slot = lax.rem(q0 + k, SLOTS)
                for j in range(TILE // SUB):
                    row = pl.multiple_of(slot * TILE + j * SUB, SUB)
                    logits = lax.dot_general(ring[pl.ds(row, SUB), :], h[lo:lo + width, :], (((1,), (1,)), ((), ())), preferred_element_type=jnp.float32)
                    reduce_logits(pending, pending_row, lo, width, keep)
                    keep = None
                    pending = logits
                    pending_row = lax.rem(q0 + k, tiles) * TILE + j * SUB
            zbuf[:, 0:width] = pending
            for k in range(GROUP):
                @pl.when(q0 + k + SLOTS < total_tiles)
                def _():
                    table_load(q0 + k + SLOTS).start()
            return carry

        lax.fori_loop(first, last, body, 0)
        if closes:
            reduce_logits(zbuf[:, 0:width], (last * GROUP % tiles or tiles) * TILE - SUB, lo, width, None)

    def stat_copy(r, device):
        return remote(stats.at[r], stats_in.at[r], stat_send.at[r], stat_recv.at[r], device)

    barrier = pltpu.get_barrier_semaphore()
    part_copy = pltpu.make_async_copy(part_hbm, part, part_sem)
    part_copy.start()
    for i in range(2 * CHUNKS):
        own_x(i).start()
    for copy in weight_loads():
        copy.start()
    for device in (to_x, to_y, to_pair):
        pl.semaphore_signal(barrier, inc=1, device_id=device, device_id_type=MESH)
    acc_sum[...] = jnp.zeros_like(acc_sum)
    acc_hit[...] = jnp.zeros_like(acc_hit)
    zbuf[...] = jnp.zeros_like(zbuf)
    stats[...] = jnp.zeros_like(stats)
    pl.semaphore_wait(barrier, 3)
    part_copy.wait()

    split = FIRST_GROUPS
    groups = tiles // GROUP
    total_tiles = tiles + split * GROUP
    scatter_start(0, 0)
    scatter_forward(0, 0)
    scatter_finish_gather_start(0, 0)
    gather_forward(0, 1)
    scatter_start(1, 0)
    gather_finish(0, 1)
    mlp(0, False)
    scatter_start(0, 2)
    scatter_forward(0, 2)
    scatter_forward(1, 0)
    scatter_finish_gather_start(0, 2)
    gather_forward(0, 3)
    scatter_finish_gather_start(1, 0)
    gather_finish(0, 3)
    pair_copy(0).start()
    gather_forward(1, 1)
    final_norm(0)
    gather_finish(1, 1)
    mlp(1, True)
    scatter_start(1, 2)
    head(0, 2, 0, 256, total_tiles, True, False)
    scatter_forward(1, 2)
    head(2, 4, 0, 256, total_tiles, False, False)
    scatter_finish_gather_start(1, 2)
    head(4, 6, 0, 256, total_tiles, False, False)
    gather_forward(1, 3)
    head(6, 8, 0, 256, total_tiles, False, False)
    gather_finish(1, 3)
    pair_copy(1).start()
    head(8, split, 0, 256, total_tiles, False, True)
    final_norm(1)
    head(split, groups, 0, 512, total_tiles, True, True)
    head(groups, groups + split, 256, 256, total_tiles, True, True)

    stats[0, 0:1, :] = jnp.sum(acc_sum[...], axis=0, keepdims=True)
    stats[0, 1:2, :] = jnp.sum(acc_hit[...], axis=0, keepdims=True)
    for r, device in enumerate((to_pair, to_x, to_y)):
        copy = stat_copy(r, device)
        copy.start()
        copy.wait_recv()
        if r < 2:
            stats[r + 1] = stats[r] + stats_in[r]
    both = stats[2] + stats_in[2]
    result = both[1:2, :] - jnp.log(both[0:1, :])
    for c in range(CHUNKS):
        for k in range(2):
            lo = (c * 2 + k) * rows
            logprob_ref[:, k * half + c * rows:k * half + (c + 1) * rows] = result[:, lo:lo + rows]

    for copy in y_copies(CHUNKS - 1):
        copy.wait()
    for r, device in enumerate((to_pair, to_x, to_y)):
        stat_copy(r, device).wait_send()
    for c in range(CHUNKS):
        drain(c, 2)
        pair_copy(c).wait_send()


def layer_head(part, x, target, g_attn_post, g_mlp_pre, g_mlp_post, g_final, w_gate, w_up, w_down, table):
    tokens, width = x.shape
    half = tokens // 2
    rows = half // CHUNKS
    f32, bf16 = jnp.float32, jnp.bfloat16
    vmem, dma = pltpu.VMEM, pltpu.SemaphoreType.DMA
    any_spec = pl.BlockSpec(memory_space=pl.ANY)
    vmem_spec = pl.BlockSpec(memory_space=pltpu.VMEM)
    gains = [g.astype(f32)[None, :] for g in (g_attn_post, g_mlp_pre, g_mlp_post, g_final)]
    ordered = target.reshape(2, CHUNKS, rows).transpose(1, 0, 2).reshape(1, tokens)
    logprob, hidden = pl.pallas_call(
        layer_head_kernel,
        in_specs=[any_spec, any_spec] + [vmem_spec] * 5 + [any_spec] * 4,
        out_specs=[vmem_spec, any_spec],
        out_shape=[jax.ShapeDtypeStruct((1, tokens), f32), jax.ShapeDtypeStruct((tokens, width), bf16)],
        scratch_shapes=[
            vmem((SLOTS * TILE, width), bf16),
            vmem((half, width), f32),
            vmem((CHUNKS, 6, BLOCK, width), f32),
            vmem((half, width), f32),
            vmem((half, width), f32),
            vmem((tokens, width), bf16),
            vmem((half, width), bf16),
            vmem((rows, width), bf16),
            vmem((rows, width), bf16),
            vmem((2 * CHUNKS, BLOCK, width), bf16),
            vmem((2 * CHUNKS, BLOCK, width), bf16),
            vmem((SUB, tokens), f32),
            vmem((8, tokens), f32),
            vmem((8, tokens), f32),
            vmem((3, 8, tokens), f32),
            vmem((3, 8, tokens), f32),
            dma((SLOTS,)),
            dma,
            dma((2 * CHUNKS,)),
            dma((CHUNKS, 2)),
            dma((4, CHUNKS, 6)),
            dma((4, CHUNKS, 6)),
            dma((CHUNKS,)),
            dma((CHUNKS,)),
            dma((3,)),
            dma((3,)),
        ],
        compiler_params=pltpu.CompilerParams(collective_id=0, has_side_effects=True, vmem_limit_bytes=66_500_000),
        name='layer_head',
    )(part, x, ordered, *gains, w_gate, w_up, w_down, table)
    return logprob.reshape(tokens), hidden


def solution(mesh):
    in_specs = (P(), P(), P(), P(), P(None, 't'), P(None, 't'), P(None, 't'), P('t', None), P(), P(), P(None, 't'), P(None, 't'), P('t', None), P(), P(), P(None, None, 't', None), P(None, None, 't', None), P(('v', 't'), None))

    def local_step(hidden_in, seq_lens, target, g_attn_pre, w_q, w_k, w_v, w_o, g_attn_post, g_mlp_pre, w_gate, w_up, w_down, g_mlp_post, g_final, k_cache, v_cache, embed_table):
        half = hidden_in.shape[0] // 2
        first = lax.axis_index('v') * half

        def mine(array):
            return lax.dynamic_slice_in_dim(array, first, half, 0)

        lens = mine(seq_lens)
        normed = rms_norm(mine(hidden_in), g_attn_pre).astype(jnp.bfloat16)
        attn_vec = attention(normed, lens, w_q, w_k, w_v, mine(k_cache), mine(v_cache))
        part = jnp.dot(attn_vec, w_o, preferred_element_type=jnp.float32)
        logprob, hidden_out = layer_head(part, hidden_in, target, g_attn_post, g_mlp_pre, g_mlp_post, g_final, w_gate, w_up, w_down, embed_table)
        return logprob, hidden_out

    return jax.shard_map(local_step, mesh=mesh, in_specs=in_specs, out_specs=(P(), P()), check_vma=False)
```

```python
import jax
import jax.numpy as jnp
import numpy as np
from jax import lax
from jax.experimental import pallas as pl
from jax.experimental.pallas import tpu as pltpu
from jax.sharding import PartitionSpec as P

ATTN_CAP = 50.0
FINAL_CAP = 30.0
NORM_EPS = 1e-6
ROPE_BASE = 10000.0
CONTEXT = 32
HEAD_DIM = 256
FIRST_GROUPS = 11
MESH = pl.DeviceIdType.MESH
BLOCK = 16
TILE = 512
SLOTS = 15
GROUP = 4
SUB = 256
CHUNKS = 2


def norm_rows(values, gain):
    return values * lax.rsqrt(jnp.mean(values * values, axis=-1, keepdims=True) + NORM_EPS) * (1.0 + gain)


def layer_head_kernel(
    lens_in, tgt_in, freq_ref, g_first_in, g_attn_in, g_pre_in, g_post_in, g_final_in,
    x_hbm, wq, wk, wv, wo, kc, vc, wg, wu, wd, table,
    logprob_ref, y_hbm,
    ring, part, landed, gat, oth, h, stage, work, x1, heads, trig, lens_ref, gains, tgt_ref,
    zbuf, acc_sum, acc_hit, stats, stats_in,
    load_sem, early_sem, y_sem, send_sem, recv_sem, pair_send, pair_recv, stat_send, stat_recv,
):
    t = lax.axis_index('t')
    v = lax.axis_index('v')
    x, y = lax.rem(t, 2), lax.div(t, 2)
    to_x = {'t': t + 1 - 2 * x}
    to_y = {'t': t + 2 - 4 * y}
    to_pair = {'v': 1 - v}
    half = part.shape[0]
    rows = half // CHUNKS
    vocab = table.shape[0]
    tiles = vocab // TILE
    base = (v * 4 + t) * vocab

    def b1(c, xo, yo):
        return c * rows + (xo * 2 + yo) * BLOCK

    def b2(c, yo, xo):
        return c * rows + rows // 2 + (yo * 2 + xo) * BLOCK

    def at(ref, row):
        return ref.at[pl.ds(pl.multiple_of(row, BLOCK), BLOCK), :]

    def remote(src, dst, send, recv, device):
        return pltpu.make_async_remote_copy(src_ref=src, dst_ref=dst, send_sem=send, recv_sem=recv, device_id=device, device_id_type=MESH)

    def weight_loads():
        out = []
        for n, w in enumerate((wg, wu, wd)):
            for k in range(5):
                slot = n * 5 + k
                out.append(pltpu.make_async_copy(w.at[pl.ds(k * TILE, TILE), :], ring.at[pl.ds(slot * TILE, TILE), :], load_sem.at[slot]))
        return out

    def table_load(q):
        slot = lax.rem(q, SLOTS)
        row = pl.multiple_of(lax.rem(q, tiles) * TILE, TILE)
        return pltpu.make_async_copy(table.at[pl.ds(row, TILE), :], ring.at[pl.ds(pl.multiple_of(slot * TILE, TILE), TILE), :], load_sem.at[slot])

    def scatter_copies(c, phase):
        s, r = send_sem.at[phase, c], recv_sem.at[phase, c]
        return (
            remote(at(part, b1(c, 1 - x, 1 - y)), landed.at[c, 0], s.at[0], r.at[0], to_x),
            remote(at(part, b1(c, 1 - x, y)), landed.at[c, 1], s.at[1], r.at[1], to_x),
            remote(at(part, b1(c, x, 1 - y)), landed.at[c, 2], s.at[2], r.at[2], to_y),
            remote(at(part, b2(c, 1 - y, 1 - x)), landed.at[c, 3], s.at[3], r.at[3], to_y),
            remote(at(part, b2(c, 1 - y, x)), landed.at[c, 4], s.at[4], r.at[4], to_y),
            remote(at(part, b2(c, y, 1 - x)), landed.at[c, 5], s.at[5], r.at[5], to_x),
        )

    def gather_copies(c, phase):
        s, r = send_sem.at[phase, c], recv_sem.at[phase, c]

        def same(row, k, device):
            return remote(at(gat, row), at(gat, row), s.at[k], r.at[k], device)

        return (
            same(b1(c, x, y), 0, to_y),
            same(b1(c, x, y), 1, to_x),
            same(b1(c, x, 1 - y), 2, to_x),
            same(b2(c, y, x), 3, to_x),
            same(b2(c, y, x), 4, to_y),
            same(b2(c, y, 1 - x), 5, to_y),
        )

    def scatter_start(c, phase):
        copies = scatter_copies(c, phase)
        for k in (0, 3, 1, 4):
            copies[k].start()

    def scatter_forward(c, phase):
        copies = scatter_copies(c, phase)
        for k, row in ((0, b1(c, x, 1 - y)), (3, b2(c, y, 1 - x))):
            copies[k].wait_recv()
            dst = at(part, row)
            dst[...] = dst[...] + landed[c, k]
            copies[k + 2].start()

    def scatter_finish_gather_start(c, phase):
        copies = scatter_copies(c, phase)
        out = gather_copies(c, phase + 1)
        for side, (k, row) in enumerate(((0, b1(c, x, y)), (3, b2(c, y, x)))):
            copies[k + 1].wait_recv()
            copies[k + 2].wait_recv()
            total = at(part, row)[...] + landed[c, k + 1] + landed[c, k + 2]
            mine = c * 2 + side
            if phase == 0:
                mid = (at(stage, row)[...].astype(jnp.float32) + norm_rows(total, gains[1:2, :])).astype(jnp.bfloat16)
                x1[mine] = mid
                value = norm_rows(mid.astype(jnp.float32), gains[2:3, :])
            else:
                value = x1[mine].astype(jnp.float32) + norm_rows(total, gains[3:4, :])
            at(gat, row)[...] = value.astype(jnp.bfloat16).astype(jnp.float32)
            out[k].start()
            out[k + 1].start()

    def gather_forward(c, phase):
        copies = gather_copies(c, phase)
        for k in (0, 3):
            copies[k].wait_recv()
            copies[k + 2].start()

    def gather_finish(c, phase):
        copies = gather_copies(c, phase)
        for k in (1, 2, 4, 5):
            copies[k].wait_recv()

    def drain(c, phase):
        for copy in scatter_copies(c, phase) + gather_copies(c, phase + 1):
            copy.wait_send()

    def early_loads():
        local = v * half
        pairs = [(x_hbm.at[pl.ds(pl.multiple_of(local, BLOCK), half), :], stage)]
        col = 0
        for w in (wq, wk, wv):
            pairs.append((w, ring.at[pl.ds(5120, 2560), pl.ds(col, w.shape[1])]))
            col += w.shape[1]
        for cache, first in ((kc, 0), (vc, 4)):
            for j in range(4):
                row = pl.multiple_of((local + j * 64) * CONTEXT, 2048)
                pairs.append((cache.at[pl.ds(row, 64 * CONTEXT), :], ring.at[pl.ds(2560, 64 * CONTEXT), pl.ds((first + j) * HEAD_DIM, HEAD_DIM)]))
        pairs.append((wo, h))
        return [pltpu.make_async_copy(src, dst, early_sem.at[i]) for i, (src, dst) in enumerate(pairs)]

    def rotate(z, c):
        low, high = z[:, 0:128], z[:, 128:256]
        cos, sin = trig[0], trig[1]
        return jnp.concatenate([low * cos - high * sin, high * cos + low * sin], axis=1)

    def project():
        early = early_loads()
        early[0].wait()

        def body(i, carry):
            row = pl.multiple_of(i * BLOCK, BLOCK)
            work[pl.ds(row, BLOCK), :] = norm_rows(stage[pl.ds(row, BLOCK), :].astype(jnp.float32), gains[0:1, :]).astype(jnp.bfloat16)
            return carry

        lax.fori_loop(0, half // BLOCK, body, 0)
        for k in (1, 2, 3):
            early[k].wait()
        for n in range(4):
            z = jnp.dot(work[...], ring[5120:7680, n * HEAD_DIM:(n + 1) * HEAD_DIM], preferred_element_type=jnp.float32)
            if n < 3:
                z = rotate(z, n)
            heads[:, n * HEAD_DIM:(n + 1) * HEAD_DIM] = z.astype(jnp.bfloat16).astype(jnp.float32)

    def attend(c):
        early = early_loads()
        for j in (2 * c, 2 * c + 1):
            early[4 + j].wait()
            early[8 + j].wait()
        shape = (16, 8 * CONTEXT)
        lane = lax.broadcasted_iota(jnp.int32, shape, 1)
        same_token = lax.rem(lax.broadcasted_iota(jnp.int32, shape, 0), 8) == lax.div(lane, CONTEXT)
        place = lax.rem(lane, CONTEXT).astype(jnp.float32)

        def twice(a):
            return jnp.concatenate([a, a], axis=0)

        def body(j, carry):
            k_cols = pl.ds(pl.multiple_of(j * HEAD_DIM, HEAD_DIM), HEAD_DIM)
            v_cols = pl.ds(pl.multiple_of((j + 4) * HEAD_DIM, HEAD_DIM), HEAD_DIM)
            for g in range(8):
                row = pl.ds(pl.multiple_of(j * 64 + g * 8, 8), 8)
                block = slice(2560 + g * 8 * CONTEXT, 2560 + (g + 1) * 8 * CONTEXT)
                q = jnp.concatenate([heads[row, 0:256], heads[row, 256:512]], axis=0)
                new_k = twice(heads[row, 512:768])
                new_v = twice(heads[row, 768:1024])
                length = twice(lens_ref[row, 0:1])
                scores = lax.dot_general(q.astype(jnp.bfloat16), ring[block, k_cols], (((1,), (1,)), ((), ())), preferred_element_type=jnp.float32)
                scores = ATTN_CAP * jnp.tanh(scores * HEAD_DIM ** -0.5 / ATTN_CAP)
                fresh = jnp.sum(q * new_k, axis=1, keepdims=True)
                fresh = ATTN_CAP * jnp.tanh(fresh * HEAD_DIM ** -0.5 / ATTN_CAP)
                scores = jnp.where(same_token & (place < length), scores, -1e30)
                top = jnp.maximum(jnp.max(scores, axis=1, keepdims=True), fresh)
                weight = jnp.exp(scores - top)
                fresh = jnp.exp(fresh - top)
                norm = jnp.sum(weight, axis=1, keepdims=True) + fresh
                mixed = jnp.dot(weight.astype(jnp.bfloat16), ring[block, v_cols], preferred_element_type=jnp.float32)
                mixed = (mixed + fresh.astype(jnp.bfloat16).astype(jnp.float32) * new_v) / norm
                heads[row, 0:256] = mixed[0:8, :]
                heads[row, 256:512] = mixed[8:16, :]
            return carry

        lax.fori_loop(2 * c, 2 * c + 2, body, 0)
        if c == 0:
            early[12].wait()
        vec = heads[c * rows:(c + 1) * rows, 0:512].astype(jnp.bfloat16)
        for n in range(5):
            cols = slice(n * TILE, (n + 1) * TILE)
            part[c * rows:(c + 1) * rows, cols] = jnp.dot(vec, h[:, cols], preferred_element_type=jnp.float32)

    def setup():
        for i, g in enumerate((g_first_in, g_attn_in, g_pre_in, g_post_in, g_final_in)):
            gains[i:i + 1, :] = g[...].astype(jnp.float32).reshape(1, g.shape[0])
        for c in range(CHUNKS):
            lens = jnp.where(v == 0, lens_in[c * rows:(c + 1) * rows], lens_in[half + c * rows:half + (c + 1) * rows])
            column = jnp.broadcast_to(lens.astype(jnp.float32).reshape(1, rows), (rows, rows)).T
            lens_ref[c * rows:(c + 1) * rows, :] = column
            angle = column * freq_ref[...]
            trig[0, c * rows:(c + 1) * rows, :] = jnp.cos(angle)
            trig[1, c * rows:(c + 1) * rows, :] = jnp.sin(angle)
            for k in range(2):
                lo = (c * 2 + k) * rows
                tgt_ref[:, lo:lo + rows] = tgt_in[k * half + c * rows:k * half + (c + 1) * rows].reshape(1, rows)

    def mlp(c, last):
        loads = weight_loads()
        work[0:rows, :] = gat[c * rows:(c + 1) * rows, :].astype(jnp.bfloat16)
        for k in range(10):
            loads[k].wait()

        def gate_up(n, carry):
            cols = pl.ds(pl.multiple_of(n * TILE, TILE), TILE)
            gate = jnp.dot(work[0:rows, :], ring[0:2560, cols], preferred_element_type=jnp.float32)
            up = jnp.dot(work[0:rows, :], ring[2560:5120, cols], preferred_element_type=jnp.float32)
            work[rows:2 * rows, cols] = (jax.nn.gelu(gate, approximate=True) * up).astype(jnp.bfloat16)
            return carry

        lax.fori_loop(0, 5, gate_up, 0)
        for k in range(10):
            if last:
                table_load(k).start(priority=1)
            else:
                loads[k].start(priority=1)
        for k in range(10, 15):
            loads[k].wait()
        drain(c, 0)

        def down(n, carry):
            cols = pl.ds(pl.multiple_of(n * TILE, TILE), TILE)
            part[c * rows:(c + 1) * rows, cols] = jnp.dot(work[rows:2 * rows, :], ring[5120:7680, cols], preferred_element_type=jnp.float32)
            return carry

        lax.fori_loop(0, 5, down, 0)
        for k in range(10, 15):
            if last:
                table_load(k).start(priority=1)
            else:
                loads[k].start(priority=1)

    def pair_copy(c):
        span = pl.ds(c * rows, rows)
        return remote(gat.at[span, :], oth.at[span, :], pair_send.at[c], pair_recv.at[c], to_pair)

    def y_copies(c):
        out = []
        for k, owner in enumerate((v, 1 - v)):
            dst = y_hbm.at[pl.ds(pl.multiple_of(owner * half + c * rows, BLOCK), rows), :]
            out.append(pltpu.make_async_copy(stage.at[pl.ds(k * rows, rows), :], dst, y_sem.at[c, k]))
        return out

    def final_norm(c):
        pair = pair_copy(c)
        if c > 0:
            for copy in y_copies(c - 1):
                copy.wait()
        for k, (src, owner) in enumerate(((gat, v), (oth, 1 - v))):
            if k == 1:
                pair.wait_recv()

            def body(i, carry):
                row = pl.multiple_of(i * BLOCK, BLOCK)
                value = src[pl.ds(c * rows + row, BLOCK), :]
                stage[pl.ds(k * rows + row, BLOCK), :] = value.astype(jnp.bfloat16)
                h[pl.ds(pl.multiple_of((c * 2 + owner) * rows + row, BLOCK), BLOCK), :] = norm_rows(value, gains[4:5, :]).astype(jnp.bfloat16)
                return carry

            lax.fori_loop(0, rows // BLOCK, body, 0)
            y_copies(c)[k].start()

    def reduce_logits(logits, first_row, lo, width, keep):
        capped = FINAL_CAP * jnp.tanh(logits / FINAL_CAP)
        row_ids = lax.broadcasted_iota(jnp.int32, logits.shape, 0)
        wanted = tgt_ref[:, lo:lo + width] - (base + first_row)
        total = jnp.sum(jnp.exp(capped).reshape(SUB // 8, 8, width), axis=0)
        hit = jnp.sum(jnp.where(row_ids == wanted, capped, 0.0).reshape(SUB // 8, 8, width), axis=0)
        if keep is not None:
            total = jnp.where(keep, total, 0.0)
            hit = jnp.where(keep, hit, 0.0)
        acc_sum[:, lo:lo + width] += total
        acc_hit[:, lo:lo + width] += hit

    def head(first, last, lo, width, total_tiles, opens, closes):
        def body(g, carry):
            q0 = g * GROUP
            for k in range(GROUP):
                table_load(q0 + k).wait()
            pending = zbuf[:, 0:width]
            pending_row = lax.rem(q0, tiles) * TILE - SUB
            keep = g > first if opens else None
            for k in range(GROUP):
                slot = lax.rem(q0 + k, SLOTS)
                for j in range(TILE // SUB):
                    row = pl.multiple_of(slot * TILE + j * SUB, SUB)
                    logits = lax.dot_general(ring[pl.ds(row, SUB), :], h[lo:lo + width, :], (((1,), (1,)), ((), ())), preferred_element_type=jnp.float32)
                    reduce_logits(pending, pending_row, lo, width, keep)
                    keep = None
                    pending = logits
                    pending_row = lax.rem(q0 + k, tiles) * TILE + j * SUB
            zbuf[:, 0:width] = pending
            for k in range(GROUP):
                @pl.when(q0 + k + SLOTS < total_tiles)
                def _():
                    table_load(q0 + k + SLOTS).start(priority=1)
            return carry

        lax.fori_loop(first, last, body, 0)
        if closes:
            reduce_logits(zbuf[:, 0:width], (last * GROUP % tiles or tiles) * TILE - SUB, lo, width, None)

    def stat_copy(r, device):
        return remote(stats.at[r], stats_in.at[r], stat_send.at[r], stat_recv.at[r], device)

    barrier = pltpu.get_barrier_semaphore()
    for copy in early_loads():
        copy.start()
    for copy in weight_loads()[0:5]:
        copy.start(priority=1)
    for device in (to_x, to_y, to_pair):
        pl.semaphore_signal(barrier, inc=1, device_id=device, device_id_type=MESH)
    acc_sum[...] = jnp.zeros_like(acc_sum)
    acc_hit[...] = jnp.zeros_like(acc_hit)
    zbuf[...] = jnp.zeros_like(zbuf)
    stats[...] = jnp.zeros_like(stats)
    setup()
    project()
    attend(0)
    pl.semaphore_wait(barrier, 3)

    split = FIRST_GROUPS
    groups = tiles // GROUP
    total_tiles = tiles + split * GROUP
    scatter_start(0, 0)
    attend(1)
    for copy in weight_loads()[5:15]:
        copy.start(priority=1)
    scatter_forward(0, 0)
    scatter_finish_gather_start(0, 0)
    gather_forward(0, 1)
    scatter_start(1, 0)
    gather_finish(0, 1)
    mlp(0, False)
    scatter_start(0, 2)
    scatter_forward(0, 2)
    scatter_forward(1, 0)
    scatter_finish_gather_start(0, 2)
    gather_forward(0, 3)
    scatter_finish_gather_start(1, 0)
    gather_finish(0, 3)
    pair_copy(0).start()
    gather_forward(1, 1)
    final_norm(0)
    gather_finish(1, 1)
    mlp(1, True)
    scatter_start(1, 2)
    head(0, 2, 0, 256, total_tiles, True, False)
    scatter_forward(1, 2)
    head(2, 4, 0, 256, total_tiles, False, False)
    scatter_finish_gather_start(1, 2)
    head(4, 6, 0, 256, total_tiles, False, False)
    gather_forward(1, 3)
    head(6, 8, 0, 256, total_tiles, False, False)
    gather_finish(1, 3)
    pair_copy(1).start()
    head(8, split, 0, 256, total_tiles, False, True)
    final_norm(1)
    head(split, groups, 0, 512, total_tiles, True, True)
    head(groups, groups + split, 256, 256, total_tiles, True, True)

    stats[0, 0:1, :] = jnp.sum(acc_sum[...], axis=0, keepdims=True)
    stats[0, 1:2, :] = jnp.sum(acc_hit[...], axis=0, keepdims=True)
    for r, device in enumerate((to_pair, to_x, to_y)):
        copy = stat_copy(r, device)
        copy.start()
        copy.wait_recv()
        if r < 2:
            stats[r + 1] = stats[r] + stats_in[r]
    both = stats[2] + stats_in[2]
    result = both[1:2, :] - jnp.log(both[0:1, :])
    for c in range(CHUNKS):
        for k in range(2):
            lo = (c * 2 + k) * rows
            logprob_ref[k * half + c * rows:k * half + (c + 1) * rows] = result[:, lo:lo + rows].reshape(rows)

    for copy in y_copies(CHUNKS - 1):
        copy.wait()
    for r, device in enumerate((to_pair, to_x, to_y)):
        stat_copy(r, device).wait_send()
    for c in range(CHUNKS):
        drain(c, 2)
        pair_copy(c).wait_send()


def layer_head(x, lens, target, g_attn_pre, w_q, w_k, w_v, w_o, g_attn_post, g_mlp_pre, w_gate, w_up, w_down, g_mlp_post, g_final, k_cache, v_cache, table):
    tokens, width = x.shape
    half = tokens // 2
    rows = half // CHUNKS
    f32, bf16 = jnp.float32, jnp.bfloat16
    vmem, dma = pltpu.VMEM, pltpu.SemaphoreType.DMA
    any_spec = pl.BlockSpec(memory_space=pl.ANY)
    vmem_spec = pl.BlockSpec(memory_space=pltpu.VMEM)
    freq = (ROPE_BASE ** (-2.0 * np.arange(HEAD_DIM // 2) / HEAD_DIM)).astype(np.float32)[None, :]
    k_rows = k_cache.reshape(tokens * CONTEXT, HEAD_DIM)
    v_rows = v_cache.reshape(tokens * CONTEXT, HEAD_DIM)
    return pl.pallas_call(
        layer_head_kernel,
        in_specs=[vmem_spec] * 8 + [any_spec] * 11,
        out_specs=[vmem_spec, any_spec],
        out_shape=[jax.ShapeDtypeStruct((tokens,), f32), jax.ShapeDtypeStruct((tokens, width), bf16)],
        scratch_shapes=[
            vmem((SLOTS * TILE, width), bf16),
            vmem((half, width), f32),
            vmem((CHUNKS, 6, BLOCK, width), f32),
            vmem((half, width), f32),
            vmem((half, width), f32),
            vmem((tokens, width), bf16),
            vmem((half, width), bf16),
            vmem((2 * rows, width), bf16),
            vmem((2 * CHUNKS, BLOCK, width), bf16),
            vmem((half, 4 * HEAD_DIM), f32),
            vmem((2, half, HEAD_DIM // 2), f32),
            vmem((half, rows), f32),
            vmem((8, width), f32),
            vmem((1, tokens), jnp.int32),
            vmem((SUB, tokens), f32),
            vmem((8, tokens), f32),
            vmem((8, tokens), f32),
            vmem((3, 8, tokens), f32),
            vmem((3, 8, tokens), f32),
            dma((SLOTS,)),
            dma((13,)),
            dma((CHUNKS, 2)),
            dma((4, CHUNKS, 6)),
            dma((4, CHUNKS, 6)),
            dma((CHUNKS,)),
            dma((CHUNKS,)),
            dma((3,)),
            dma((3,)),
        ],
        compiler_params=pltpu.CompilerParams(collective_id=0, has_side_effects=True, vmem_limit_bytes=66_500_000),
        name='layer_head',
    )(lens, target, freq, g_attn_pre, g_attn_post, g_mlp_pre, g_mlp_post, g_final, x, w_q, w_k, w_v, w_o, k_rows, v_rows, w_gate, w_up, w_down, table)


def solution(mesh):
    in_specs = (P(), P(), P(), P(), P(None, 't'), P(None, 't'), P(None, 't'), P('t', None), P(), P(), P(None, 't'), P(None, 't'), P('t', None), P(), P(), P(None, None, 't', None), P(None, None, 't', None), P(('v', 't'), None))
    return jax.shard_map(layer_head, mesh=mesh, in_specs=in_specs, out_specs=(P(), P()), check_vma=False)
```
